128 devices in a mesh: lat: 16 (over z_hi, y_lo, x), lon: 4 (over z_lo, core), lev: 2 (over y_hi).
Axes of the slice: x: 4, y: 4 (y_hi: 2, y_lo: 2; y = y_hi * 2 + y_lo), z: 4 (z_hi: 2, z_lo: 2; z = z_hi * 2 + z_lo), core: 2. Of those that a mesh axis runs over, the one named last changes fastest.
Arguments:
- field_values: float32 [64, 256, 192, 128], P('lat', 'lon', 'lev'), may hold values from 0.2 to 1.8
- crowding: float32 [64, 256, 192, 128], P('lat', 'lon', 'lev'), may hold values from 0.5 to 2
Outputs:
- field_values_end: float32 [64, 256, 192, 128], P('lat', 'lon', 'lev')
The draws below stay inside these ranges and needn't reach their ends.
All inputs are finite; a program needn't handle non-finite values.
Results may differ from the reference program's by a relative error of at most 0.00002.
Values sent between devices are 32-bit elements; how exact they have to be, the bound alone decides.
A program may use at most 384 MiB of HBM per device.

```python
import jax
import jax.numpy as jnp
from jax import lax

GRID_J = 64
GRID_I = 256
GRID_K = 192
LEVELS = 128
STEPS = 3


def level_of(stream_key, shape, pieces, least, top_value):
    def one(axis_at, shards_of):
        heights = jax.random.uniform(jax.random.fold_in(jax.random.fold_in(stream_key, 6), axis_at), (shards_of,), jnp.float32, least / len(pieces), top_value / len(pieces))
        return jnp.repeat(jnp.exp(heights), shape[axis_at] // shards_of).reshape((-1,) + (1,) * (len(shape) - axis_at - 1))

    level = one(*pieces[0])
    for cut in pieces[1:]:
        level = level * one(*cut)
    return level


def setup_inputs(seed: int = 0) -> dict:
    arg_keys = jax.random.split(jax.random.key(seed), 3)
    field_values = jnp.clip(0.2 + 1.5999999 * jax.random.uniform(arg_keys[0], (GRID_J, GRID_I, GRID_K, LEVELS), jnp.float32) ** level_of(arg_keys[0], (GRID_J, GRID_I, GRID_K, LEVELS), ((0, 16), (1, 4), (2, 2)), -0.2, 0.2), 0.2, 1.8)
    crowding = jnp.clip(0.5 + 1.5 * jax.random.uniform(arg_keys[1], (GRID_J, GRID_I, GRID_K, LEVELS), jnp.float32) ** level_of(arg_keys[1], (GRID_J, GRID_I, GRID_K, LEVELS), ((0, 16), (1, 4), (2, 2)), -0.2, 0.2), 0.5, 2.0)
    return {"field_values": field_values, "crowding": crowding}


def without_rim(values, dims):
    for dim in dims:
        values = lax.slice_in_dim(values, 1, values.shape[dim] - 1, axis=dim)
    return values


def shifted_cells(values, dim, start, dims):
    others = [other for other in dims if other != dim]
    values = without_rim(values, others)
    return lax.slice_in_dim(values, start, start + values.shape[dim] - 2, axis=dim)


def march_step(padded, crowding):
    middle = without_rim(padded, (0, 1, 2))
    lower = [shifted_cells(padded, dim, 0, (0, 1, 2)) for dim in (0, 1, 2)]
    upper = [shifted_cells(padded, dim, 2, (0, 1, 2)) for dim in (0, 1, 2)]
    spread = lower[0] + upper[0] + lower[1] + upper[1] + lower[2] + upper[2] - 6.0 * middle
    return middle + 0.1 * spread + 0.2 * middle * (1.0 - middle * crowding)


def reference(field_values, crowding):
    for step in range(STEPS):
        field_values = march_step(jnp.pad(field_values, ((1, 1), (1, 1), (1, 1), (0, 0)), mode="wrap"), crowding)
    return field_values
```

```python
import functools

import jax
import jax.numpy as jnp
from jax import lax
from jax.experimental import pallas as pl
from jax.experimental.pallas import tpu as pltpu
from jax.sharding import PartitionSpec as P

STEPS = 3
ROWS = 4
AHEAD = 3
GROUPS = 4
LOW, HIGH = 0, 1


def kernel(
    field, crowding, out,
    even, odd, crowd, lat_halo, lev_face, lev_halo,
    load_sem, out_sem, lat_send, lat_recv, lon_send, lon_recv, lev_send, lev_recv,
):
    depth, width, tall, _ = field.shape
    chunks = width // ROWS
    each = chunks // GROUPS
    bufs = (even, odd)

    def beside(axis, step):
        size = lax.axis_size(axis)
        return {axis: lax.rem(lax.axis_index(axis) + step + size, size)}

    lat_at = (beside("lat", -1), beside("lat", 1))
    lon_at = (beside("lon", -1), beside("lon", 1))
    lev_at = (beside("lev", -1), beside("lev", 1))

    def chunk_at(n):
        return jnp.where(n == 0, 0, jnp.where(n == 1, chunks - 1, n - 1))

    load_field = pltpu.make_async_copy(field, even.at[:, pl.ds(1, width)], load_sem.at[0])
    load_crowd = pltpu.make_async_copy(crowding, crowd, load_sem.at[1])

    def lat_copy(t, side, n):
        plane = depth - 1 if side == LOW else 0
        rows = chunk_at(n) * ROWS
        if t == 0:
            src = field.at[plane, pl.ds(rows, ROWS)]
        else:
            src = bufs[t % 2].at[plane, pl.ds(rows + 1, ROWS)]
        return pltpu.make_async_remote_copy(
            src_ref=src,
            dst_ref=lat_halo.at[t % 2, side, pl.ds(rows, ROWS)],
            send_sem=lat_send.at[side, n],
            recv_sem=lat_recv.at[t % 2, side, n],
            device_id=lat_at[1 - side],
            device_id_type=pl.DeviceIdType.MESH,
        )

    def lon_copy(t, side):
        row = width - 1 if side == LOW else 0
        src = field.at[:, row] if t == 0 else bufs[t % 2].at[:, row + 1]
        return pltpu.make_async_remote_copy(
            src_ref=src,
            dst_ref=bufs[t % 2].at[:, 0 if side == LOW else width + 1],
            send_sem=lon_send.at[t, side],
            recv_sem=lon_recv.at[t, side],
            device_id=lon_at[1 - side],
            device_id_type=pl.DeviceIdType.MESH,
        )

    def lev_copy(t, side, group):
        rows = pl.ds(group * (each * ROWS), each * ROWS)
        return pltpu.make_async_remote_copy(
            src_ref=lev_face.at[t, side, rows],
            dst_ref=lev_halo.at[t, side, rows],
            send_sem=lev_send.at[t, side, group],
            recv_sem=lev_recv.at[t, side, group],
            device_id=lev_at[1 - side],
            device_id_type=pl.DeviceIdType.MESH,
        )

    def out_copy(n):
        rows = chunk_at(n) * ROWS
        return pltpu.make_async_copy(
            odd.at[:, pl.ds(rows + 1, ROWS)], out.at[:, pl.ds(rows, ROWS)], out_sem.at[n]
        )

    def both(copy, *where):
        return [copy(*(where[:1] + (side,) + where[1:])) for side in (LOW, HIGH)]

    load_field.start()
    load_crowd.start()
    barrier = pltpu.get_barrier_semaphore()
    partners = (*lat_at, *lon_at, lev_at[0])
    for partner in partners:
        pl.semaphore_signal(barrier, inc=1, device_id=partner, device_id_type=pl.DeviceIdType.MESH)
    pl.semaphore_wait(barrier, len(partners))

    for n in range(AHEAD):
        for copy in both(lat_copy, 0, n):
            copy.start()
    for copy in both(lon_copy, 0):
        copy.start()
    load_field.wait()

    def pack(position, carry):
        n = position // ROWS
        row = chunk_at(n) * ROWS + position % ROWS + 1
        for plane in range(depth):
            lev_face[0, LOW, position, pl.ds(plane, 1)] = even[plane, row, pl.ds(tall - 1, 1)]
            lev_face[0, HIGH, position, pl.ds(plane, 1)] = even[plane, row, pl.ds(0, 1)]
        return carry

    lax.fori_loop(0, width, pack, 0)
    for group in range(GROUPS):
        for copy in both(lev_copy, 0, group):
            copy.start()
    load_crowd.wait()

    edge = lax.broadcasted_iota(jnp.int32, (8, 128), 0)

    def new_row(s, n, r):
        src, dst = bufs[s % 2], bufs[(s + 1) % 2]
        at = chunk_at(n) * ROWS + r
        row, position = at + 1, n * ROWS + r
        for plane in range(depth):
            for start, stop in ((0, 8), (8, 32), (32, 64), (64, tall - 8), (tall - 8, tall)):
                span = pl.ds(start, stop - start)
                middle = src[plane, row, span]
                if start == 0:
                    halo = lev_halo[s, LOW, position, pl.ds(plane, 1)]
                    lower = jnp.where(edge == 0, halo, pltpu.roll(middle, 1, 0))
                else:
                    lower = src[plane, row, pl.ds(start - 1, stop - start)]
                if stop == tall:
                    halo = lev_halo[s, HIGH, position, pl.ds(plane, 1)]
                    upper = jnp.where(edge == 7, halo, pltpu.roll(middle, 7, 0))
                else:
                    upper = src[plane, row, pl.ds(start + 1, stop - start)]
                around = lower + upper + src[plane, row - 1, span] + src[plane, row + 1, span]
                if plane == 0:
                    around += lat_halo[s % 2, LOW, at, span]
                else:
                    around += src[plane - 1, row, span]
                if plane == depth - 1:
                    around += lat_halo[s % 2, HIGH, at, span]
                else:
                    around += src[plane + 1, row, span]
                growth = 0.6 - 0.2 * (middle * crowd[plane, at, span])
                new = 0.1 * around + middle * growth
                dst[plane, row, span] = new
                if s < STEPS - 1:
                    if start == 0:
                        lev_face[s + 1, HIGH, position, pl.ds(plane, 1)] = new[0:1]
                    if stop == tall:
                        lev_face[s + 1, LOW, position, pl.ds(plane, 1)] = new[7:8]

    for s in range(STEPS):

        def chunk(n, carry, s=s):
            for copy in both(lat_copy, s, n):
                copy.wait_recv()

            @pl.when(n + AHEAD < chunks)
            def _():
                if s > 0:
                    for copy in both(lat_copy, s - 1, n + AHEAD):
                        copy.wait_send()
                for copy in both(lat_copy, s, n + AHEAD):
                    copy.start()

            if s < STEPS - 1:

                @pl.when(n + AHEAD >= chunks)
                def _():
                    for copy in both(lat_copy, s, n + AHEAD - chunks):
                        copy.wait_send()
                    for copy in both(lat_copy, s + 1, n + AHEAD - chunks):
                        copy.start()

            @pl.when(n == 0)
            def _():
                if s > 0:
                    for copy in both(lev_copy, s, GROUPS - 1):
                        copy.start()
                    for copy in both(lon_copy, s - 1):
                        copy.wait_send()
                for copy in both(lon_copy, s):
                    copy.wait_recv()

            if s < STEPS - 1:

                @pl.when(n == 2)
                def _():
                    for copy in both(lon_copy, s + 1):
                        copy.start()

            @pl.when(n % each == 0)
            def _():
                for copy in both(lev_copy, s, n // each):
                    copy.wait_recv()
                if s < STEPS - 1:

                    @pl.when(n > 0)
                    def _():
                        for copy in both(lev_copy, s + 1, n // each - 1):
                            copy.start()

            if s == STEPS - 1:

                @pl.when(n > 0)
                def _():
                    out_copy(n - 1).start()

            def row(r, inner):
                new_row(s, n, r)
                return inner

            return lax.fori_loop(0, ROWS, row, carry)

        lax.fori_loop(0, chunks, chunk, 0)

    out_copy(chunks - 1).start()

    def drain(n, carry):
        for copy in both(lat_copy, STEPS - 1, n):
            copy.wait_send()
        out_copy(n).wait()
        return carry

    for copy in both(lon_copy, STEPS - 1):
        copy.wait_send()
    for t in range(STEPS):
        for group in range(GROUPS):
            for copy in both(lev_copy, t, group):
                copy.wait_send()
    lax.fori_loop(0, chunks, drain, 0)


def local(field, crowding):
    depth, width, tall, lanes = field.shape
    chunks = width // ROWS
    padded = (depth, width + 2, tall, lanes)
    faces = (STEPS, 2, width, depth, lanes)
    dma = pltpu.SemaphoreType.DMA
    return pl.pallas_call(
        kernel,
        out_shape=jax.ShapeDtypeStruct(field.shape, field.dtype),
        in_specs=[pl.BlockSpec(memory_space=pl.ANY)] * 2,
        out_specs=pl.BlockSpec(memory_space=pl.ANY),
        scratch_shapes=[
            pltpu.VMEM(padded, jnp.float32),
            pltpu.VMEM(padded, jnp.float32),
            pltpu.VMEM(field.shape, jnp.float32),
            pltpu.VMEM((2, 2, width, tall, lanes), jnp.float32),
            pltpu.VMEM(faces, jnp.float32),
            pltpu.VMEM(faces, jnp.float32),
            dma((2,)),
            dma((chunks,)),
            dma((2, chunks)),
            dma((2, 2, chunks)),
            dma((STEPS, 2)),
            dma((STEPS, 2)),
            dma((STEPS, 2, GROUPS)),
            dma((STEPS, 2, GROUPS)),
        ],
        compiler_params=pltpu.CompilerParams(
            collective_id=0, has_side_effects=True, vmem_limit_bytes=60 * 1024 * 1024
        ),
        name="march",
    )(field, crowding)


def solution(mesh):
    spec = P("lat", "lon", "lev", None)
    return jax.shard_map(
        local, mesh=mesh, in_specs=(spec, spec), out_specs=spec, check_vma=False
    )
```

```python
import functools

import jax
import jax.numpy as jnp
from jax import lax
from jax.experimental import pallas as pl
from jax.experimental.pallas import tpu as pltpu
from jax.sharding import PartitionSpec as P

STEPS = 3
ROWS = 2
AHEAD = 16
LEADS = (8, 6)
SETTLE = 6
DIRECT = 12
GROUPS = 4
LOW, HIGH = 0, 1


def kernel(
    field, crowding, out,
    even, odd, crowd, lat_halo, lev_face, lev_halo, relay,
    load_sem, out_sem, lat_send, lat_recv, lon_send, lon_recv, lev_send, lev_recv,
    relay_send, relay_recv,
):
    depth, width, tall, _ = field.shape
    chunks = width // ROWS
    each = chunks // GROUPS
    bufs = (even, odd)

    def beside(axis, step):
        size = lax.axis_size(axis)
        return {axis: lax.rem(lax.axis_index(axis) + step + size, size)}

    lat_at = (beside("lat", -1), beside("lat", 1))
    lon_at = (beside("lon", -1), beside("lon", 1))
    lev_at = (beside("lev", -1), beside("lev", 1))

    lat = lax.axis_index("lat")
    x, y = lat % 4, (lat // 4) % 2
    first, last = x == 0, x == 3
    edge = first | last
    corner = (first & (y == 0)) | (last & (y == 1))
    mine = jnp.where(first, LOW, HIGH)
    across = {"lat": jnp.where(first, lat + 3, jnp.where(last, lat - 3, lat))}
    turned = {"lat": jnp.where(y == 0, lat + 4, lat - 4)}
    lifted = {"lat": lax.rem(lat + 8, 16)}

    def chunk_at(n):
        return jnp.where(n == 0, 0, jnp.where(n == 1, chunks - 1, n - 1))

    load_field = pltpu.make_async_copy(field, even.at[:, pl.ds(1, width)], load_sem.at[0])
    load_crowd = pltpu.make_async_copy(crowding, crowd, load_sem.at[1])

    def lat_copy(t, side, n):
        plane = depth - 1 if side == LOW else 0
        rows = chunk_at(n) * ROWS
        if t == 0:
            src = field.at[plane, pl.ds(rows, ROWS)]
        else:
            src = bufs[t % 2].at[plane, pl.ds(rows + 1, ROWS)]
        return pltpu.make_async_remote_copy(
            src_ref=src,
            dst_ref=lat_halo.at[t % 2, side, pl.ds(rows, ROWS)],
            send_sem=lat_send.at[side, n],
            recv_sem=lat_recv.at[t % 2, side, n],
            device_id=lat_at[1 - side],
            device_id_type=pl.DeviceIdType.MESH,
        )

    def lat_start(t, side, n):
        plain = lat_copy(t, side, n)
        leaves = last if side == LOW else first
        if t == STEPS - 1:
            leaves = leaves & (n < DIRECT)

        @pl.when(leaves)
        def _():
            pltpu.make_async_remote_copy(
                src_ref=plain.src_ref,
                dst_ref=relay.at[0, pl.ds(chunk_at(n) * ROWS, ROWS)],
                send_sem=lat_send.at[side, n],
                recv_sem=relay_recv.at[0, n],
                device_id=across,
                device_id_type=pl.DeviceIdType.MESH,
            ).start()

        @pl.when(jnp.logical_not(leaves))
        def _():
            plain.start()

    def relay_copy(t, stage, n, arrives):
        rows = pl.ds(chunk_at(n) * ROWS, ROWS)
        return pltpu.make_async_remote_copy(
            src_ref=relay.at[stage, rows],
            dst_ref=lat_halo.at[t % 2, mine, rows] if arrives else relay.at[1, rows],
            send_sem=relay_send.at[stage, n],
            recv_sem=lat_recv.at[t % 2, mine, n] if arrives else relay_recv.at[1, n],
            device_id=lifted if stage else turned,
            device_id_type=pl.DeviceIdType.MESH,
        )

    def relay_landed(stage, n):
        rows = pl.ds(chunk_at(n) * ROWS, ROWS)
        pltpu.make_async_remote_copy(
            src_ref=relay.at[stage, rows],
            dst_ref=relay.at[stage, rows],
            send_sem=relay_send.at[stage, n],
            recv_sem=relay_recv.at[stage, n],
            device_id=lifted,
            device_id_type=pl.DeviceIdType.MESH,
        ).wait_recv()

    def send_on(t, stage, n):
        relay_landed(stage, n)
        if stage == 1:
            relay_copy(t, stage, n, True).start()
            return

        @pl.when(corner)
        def _():
            relay_copy(t, stage, n, True).start()

        @pl.when(jnp.logical_not(corner))
        def _():
            relay_copy(t, stage, n, False).start()

    def relays(s, n):
        for stage, (lead, there) in enumerate(zip(LEADS, (edge, corner))):
            ahead = n + lead
            here = there & (ahead < (DIRECT if s == STEPS - 1 else chunks))

            @pl.when(here)
            def _():
                send_on(s, stage, ahead)

            if s < STEPS - 1:
                end = DIRECT if s + 1 == STEPS - 1 else chunks

                @pl.when(there & (ahead >= chunks) & (ahead - chunks < end))
                def _():
                    send_on(s + 1, stage, ahead - chunks)

            left = n - SETTLE

            @pl.when(there & (left >= 0) & (left < (DIRECT if s == STEPS - 1 else chunks)))
            def _():
                relay_copy(s, stage, left, True).wait_send()

            if s > 0:

                @pl.when(there & (left < 0))
                def _():
                    relay_copy(s - 1, stage, left + chunks, True).wait_send()

    def lon_copy(t, side):
        row = width - 1 if side == LOW else 0
        src = field.at[:, row] if t == 0 else bufs[t % 2].at[:, row + 1]
        return pltpu.make_async_remote_copy(
            src_ref=src,
            dst_ref=bufs[t % 2].at[:, 0 if side == LOW else width + 1],
            send_sem=lon_send.at[t, side],
            recv_sem=lon_recv.at[t, side],
            device_id=lon_at[1 - side],
            device_id_type=pl.DeviceIdType.MESH,
        )

    def lev_copy(t, side, group):
        rows = pl.ds(group * (each * ROWS), each * ROWS)
        return pltpu.make_async_remote_copy(
            src_ref=lev_face.at[t, side, rows],
            dst_ref=lev_halo.at[t, side, rows],
            send_sem=lev_send.at[t, side, group],
            recv_sem=lev_recv.at[t, side, group],
            device_id=lev_at[1 - side],
            device_id_type=pl.DeviceIdType.MESH,
        )

    def out_copy(n):
        rows = chunk_at(n) * ROWS
        return pltpu.make_async_copy(
            odd.at[:, pl.ds(rows + 1, ROWS)], out.at[:, pl.ds(rows, ROWS)], out_sem.at[n]
        )

    def both(copy, *where):
        return [copy(*(where[:1] + (side,) + where[1:])) for side in (LOW, HIGH)]

    load_field.start()
    load_crowd.start()
    barrier = pltpu.get_barrier_semaphore()

    def greet(partners):
        for partner in partners:
            pl.semaphore_signal(
                barrier, inc=1, device_id=partner, device_id_type=pl.DeviceIdType.MESH
            )

    greet((*lat_at, *lon_at, lev_at[0]))

    @pl.when(edge)
    def _():
        greet((across, turned, lifted))

    pl.semaphore_wait(barrier, jnp.where(edge, 8, 5))

    for copy in both(lon_copy, 0):
        copy.start()

    def launch(n, carry):
        for side in (LOW, HIGH):
            lat_start(0, side, n)
        return carry

    lax.fori_loop(0, AHEAD, launch, 0)
    load_field.wait()

    def pack(position, carry):
        n = position // ROWS
        row = chunk_at(n) * ROWS + position % ROWS + 1
        for plane in range(depth):
            lev_face[0, LOW, position, pl.ds(plane, 1)] = even[plane, row, pl.ds(tall - 1, 1)]
            lev_face[0, HIGH, position, pl.ds(plane, 1)] = even[plane, row, pl.ds(0, 1)]
        return carry

    lax.fori_loop(0, width, pack, 0)
    for group in range(GROUPS):
        for copy in both(lev_copy, 0, group):
            copy.start()
    load_crowd.wait()

    for stage, (lead, there) in enumerate(zip(LEADS, (edge, corner))):

        @pl.when(there)
        def _(stage=stage, lead=lead):
            def begin(n, carry):
                send_on(0, stage, n)
                return carry

            lax.fori_loop(0, lead, begin, 0)

    place = lax.broadcasted_iota(jnp.int32, (8, 128), 0)

    def new_row(s, n, r):
        src, dst = bufs[s % 2], bufs[(s + 1) % 2]
        at = chunk_at(n) * ROWS + r
        row, position = at + 1, n * ROWS + r
        for plane in range(depth):
            for start, stop in ((0, 8), (8, 32), (32, 64), (64, tall - 8), (tall - 8, tall)):
                span = pl.ds(start, stop - start)
                middle = src[plane, row, span]
                if start == 0:
                    halo = lev_halo[s, LOW, position, pl.ds(plane, 1)]
                    lower = jnp.where(place == 0, halo, pltpu.roll(middle, 1, 0))
                else:
                    lower = src[plane, row, pl.ds(start - 1, stop - start)]
                if stop == tall:
                    halo = lev_halo[s, HIGH, position, pl.ds(plane, 1)]
                    upper = jnp.where(place == 7, halo, pltpu.roll(middle, 7, 0))
                else:
                    upper = src[plane, row, pl.ds(start + 1, stop - start)]
                around = lower + upper + src[plane, row - 1, span] + src[plane, row + 1, span]
                if plane == 0:
                    around += lat_halo[s % 2, LOW, at, span]
                else:
                    around += src[plane - 1, row, span]
                if plane == depth - 1:
                    around += lat_halo[s % 2, HIGH, at, span]
                else:
                    around += src[plane + 1, row, span]
                growth = 0.6 - 0.2 * (middle * crowd[plane, at, span])
                new = 0.1 * around + middle * growth
                dst[plane, row, span] = new
                if s < STEPS - 1:
                    if start == 0:
                        lev_face[s + 1, HIGH, position, pl.ds(plane, 1)] = new[0:1]
                    if stop == tall:
                        lev_face[s + 1, LOW, position, pl.ds(plane, 1)] = new[7:8]

    for s in range(STEPS):

        def chunk(n, carry, s=s):
            relays(s, n)
            for copy in both(lat_copy, s, n):
                copy.wait_recv()

            @pl.when(n + AHEAD < chunks)
            def _():
                if s > 0:
                    for copy in both(lat_copy, s - 1, n + AHEAD):
                        copy.wait_send()
                for side in (LOW, HIGH):
                    lat_start(s, side, n + AHEAD)

            if s < STEPS - 1:

                @pl.when(n + AHEAD >= chunks)
                def _():
                    for copy in both(lat_copy, s, n + AHEAD - chunks):
                        copy.wait_send()
                    for side in (LOW, HIGH):
                        lat_start(s + 1, side, n + AHEAD - chunks)

            @pl.when(n == 0)
            def _():
                if s > 0:
                    for copy in both(lev_copy, s, GROUPS - 1):
                        copy.start()
                    for copy in both(lon_copy, s - 1):
                        copy.wait_send()
                for copy in both(lon_copy, s):
                    copy.wait_recv()

            if s < STEPS - 1:

                @pl.when(n == 2)
                def _():
                    for copy in both(lon_copy, s + 1):
                        copy.start()

            @pl.when(n % each == 0)
            def _():
                for copy in both(lev_copy, s, n // each):
                    copy.wait_recv()
                if s < STEPS - 1:

                    @pl.when(n > 0)
                    def _():
                        for copy in both(lev_copy, s + 1, n // each - 1):
                            copy.start()

            if s == STEPS - 1:

                @pl.when(n > 0)
                def _():
                    out_copy(n - 1).start()

            def row(r, inner):
                new_row(s, n, r)
                return inner

            return lax.fori_loop(0, ROWS, row, carry)

        lax.fori_loop(0, chunks, chunk, 0)

    out_copy(chunks - 1).start()

    def drain(n, carry):
        for copy in both(lat_copy, STEPS - 1, n):
            copy.wait_send()
        out_copy(n).wait()
        return carry

    for copy in both(lon_copy, STEPS - 1):
        copy.wait_send()
    for t in range(STEPS):
        for group in range(GROUPS):
            for copy in both(lev_copy, t, group):
                copy.wait_send()
    lax.fori_loop(0, chunks, drain, 0)


def local(field, crowding):
    depth, width, tall, lanes = field.shape
    chunks = width // ROWS
    padded = (depth, width + 2, tall, lanes)
    faces = (STEPS, 2, width, depth, lanes)
    dma = pltpu.SemaphoreType.DMA
    return pl.pallas_call(
        kernel,
        out_shape=jax.ShapeDtypeStruct(field.shape, field.dtype),
        in_specs=[pl.BlockSpec(memory_space=pl.ANY)] * 2,
        out_specs=pl.BlockSpec(memory_space=pl.ANY),
        scratch_shapes=[
            pltpu.VMEM(padded, jnp.float32),
            pltpu.VMEM(padded, jnp.float32),
            pltpu.VMEM(field.shape, jnp.float32),
            pltpu.VMEM((2, 2, width, tall, lanes), jnp.float32),
            pltpu.VMEM(faces, jnp.float32),
            pltpu.VMEM(faces, jnp.float32),
            pltpu.VMEM((2, width, tall, lanes), jnp.float32),
            dma((2,)),
            dma((chunks,)),
            dma((2, chunks)),
            dma((2, 2, chunks)),
            dma((STEPS, 2)),
            dma((STEPS, 2)),
            dma((STEPS, 2, GROUPS)),
            dma((STEPS, 2, GROUPS)),
            dma((2, chunks)),
            dma((2, chunks)),
        ],
        compiler_params=pltpu.CompilerParams(
            collective_id=0, has_side_effects=True, vmem_limit_bytes=60 * 1024 * 1024
        ),
        name="march",
    )(field, crowding)


def solution(mesh):
    spec = P("lat", "lon", "lev", None)
    return jax.shard_map(
        local, mesh=mesh, in_specs=(spec, spec), out_specs=spec, check_vma=False
    )
```

```python
import functools

import jax
import jax.numpy as jnp
from jax import lax
from jax.experimental import pallas as pl
from jax.experimental.pallas import tpu as pltpu
from jax.sharding import PartitionSpec as P

STEPS = 3
ROWS = 2
AHEAD = 12
LEADS = (4, 2)
SETTLE = 6
DIRECT = 32
GROUPS = 4
LOW, HIGH = 0, 1


def kernel(
    field, crowding, crowd,
    even, odd, lat_halo, lev_face, lev_halo, relay,
    load_sem, lat_send, lat_recv, lon_send, lon_recv, lev_send, lev_recv,
    relay_send, relay_recv,
):
    depth, width, tall, _ = field.shape
    chunks = width // ROWS
    each = chunks // GROUPS
    bufs = (even, odd)

    def beside(axis, step):
        size = lax.axis_size(axis)
        return {axis: lax.rem(lax.axis_index(axis) + step + size, size)}

    lat_at = (beside("lat", -1), beside("lat", 1))
    lon_at = (beside("lon", -1), beside("lon", 1))
    lev_at = (beside("lev", -1), beside("lev", 1))

    lat = lax.axis_index("lat")
    x, y = lat % 4, (lat // 4) % 2
    first, last = x == 0, x == 3
    edge = first | last
    corner = (first & (y == 0)) | (last & (y == 1))
    mine = jnp.where(first, LOW, HIGH)
    across = {"lat": jnp.where(first, lat + 3, jnp.where(last, lat - 3, lat))}
    turned = {"lat": jnp.where(y == 0, lat + 4, lat - 4)}
    lifted = {"lat": lax.rem(lat + 8, 16)}

    def chunk_at(n):
        return jnp.where(n == 0, 0, jnp.where(n == 1, chunks - 1, n - 1))

    load_field = pltpu.make_async_copy(field, even.at[:, pl.ds(1, width)], load_sem.at[0])
    load_crowd = pltpu.make_async_copy(crowding, crowd, load_sem.at[1])

    def lat_copy(t, side, n):
        plane = depth - 1 if side == LOW else 0
        rows = chunk_at(n) * ROWS
        if t == 0:
            src = field.at[plane, pl.ds(rows, ROWS)]
        else:
            src = bufs[t % 2].at[plane, pl.ds(rows + 1, ROWS)]
        return pltpu.make_async_remote_copy(
            src_ref=src,
            dst_ref=lat_halo.at[t % 2, side, pl.ds(rows, ROWS)],
            send_sem=lat_send.at[side, n],
            recv_sem=lat_recv.at[t % 2, side, n],
            device_id=lat_at[1 - side],
            device_id_type=pl.DeviceIdType.MESH,
        )

    def lat_start(t, side, n):
        plain = lat_copy(t, side, n)
        leaves = last if side == LOW else first
        if t == STEPS - 1:
            leaves = leaves & (n < DIRECT)

        @pl.when(leaves)
        def _():
            pltpu.make_async_remote_copy(
                src_ref=plain.src_ref,
                dst_ref=relay.at[0, pl.ds(chunk_at(n) * ROWS, ROWS)],
                send_sem=lat_send.at[side, n],
                recv_sem=relay_recv.at[0, n],
                device_id=across,
                device_id_type=pl.DeviceIdType.MESH,
            ).start()

        @pl.when(jnp.logical_not(leaves))
        def _():
            plain.start()

    def relay_copy(t, stage, n, arrives):
        rows = pl.ds(chunk_at(n) * ROWS, ROWS)
        return pltpu.make_async_remote_copy(
            src_ref=relay.at[stage, rows],
            dst_ref=lat_halo.at[t % 2, mine, rows] if arrives else relay.at[1, rows],
            send_sem=relay_send.at[stage, n],
            recv_sem=lat_recv.at[t % 2, mine, n] if arrives else relay_recv.at[1, n],
            device_id=lifted if stage else turned,
            device_id_type=pl.DeviceIdType.MESH,
        )

    def relay_landed(stage, n):
        rows = pl.ds(chunk_at(n) * ROWS, ROWS)
        pltpu.make_async_remote_copy(
            src_ref=relay.at[stage, rows],
            dst_ref=relay.at[stage, rows],
            send_sem=relay_send.at[stage, n],
            recv_sem=relay_recv.at[stage, n],
            device_id=lifted,
            device_id_type=pl.DeviceIdType.MESH,
        ).wait_recv()

    def send_on(t, stage, n):
        relay_landed(stage, n)
        if stage == 1:
            relay_copy(t, stage, n, True).start()
            return

        @pl.when(corner)
        def _():
            relay_copy(t, stage, n, True).start()

        @pl.when(jnp.logical_not(corner))
        def _():
            relay_copy(t, stage, n, False).start()

    def relays(s, n):
        for stage, (lead, there) in enumerate(zip(LEADS, (edge, corner))):
            ahead = n + lead
            here = there & (ahead < (DIRECT if s == STEPS - 1 else chunks))

            @pl.when(here)
            def _():
                send_on(s, stage, ahead)

            if s < STEPS - 1:
                end = DIRECT if s + 1 == STEPS - 1 else chunks

                @pl.when(there & (ahead >= chunks) & (ahead - chunks < end))
                def _():
                    send_on(s + 1, stage, ahead - chunks)

            left = n - SETTLE

            @pl.when(there & (left >= 0) & (left < (DIRECT if s == STEPS - 1 else chunks)))
            def _():
                relay_copy(s, stage, left, True).wait_send()

            if s > 0:

                @pl.when(there & (left < 0))
                def _():
                    relay_copy(s - 1, stage, left + chunks, True).wait_send()

    def lon_copy(t, side):
        row = width - 1 if side == LOW else 0
        src = field.at[:, row] if t == 0 else bufs[t % 2].at[:, row + 1]
        return pltpu.make_async_remote_copy(
            src_ref=src,
            dst_ref=bufs[t % 2].at[:, 0 if side == LOW else width + 1],
            send_sem=lon_send.at[t, side],
            recv_sem=lon_recv.at[t, side],
            device_id=lon_at[1 - side],
            device_id_type=pl.DeviceIdType.MESH,
        )

    def lev_copy(t, side, group):
        rows = pl.ds(group * (each * ROWS), each * ROWS)
        return pltpu.make_async_remote_copy(
            src_ref=lev_face.at[t, side, rows],
            dst_ref=lev_halo.at[t, side, rows],
            send_sem=lev_send.at[t, side, group],
            recv_sem=lev_recv.at[t, side, group],
            device_id=lev_at[1 - side],
            device_id_type=pl.DeviceIdType.MESH,
        )

    def both(copy, *where):
        return [copy(*(where[:1] + (side,) + where[1:])) for side in (LOW, HIGH)]

    load_field.start()
    load_crowd.start()
    barrier = pltpu.get_barrier_semaphore()

    def greet(partners):
        for partner in partners:
            pl.semaphore_signal(
                barrier, inc=1, device_id=partner, device_id_type=pl.DeviceIdType.MESH
            )

    greet((*lat_at, *lon_at, lev_at[0]))

    @pl.when(edge)
    def _():
        greet((across, turned, lifted))

    pl.semaphore_wait(barrier, jnp.where(edge, 8, 5))

    for copy in both(lon_copy, 0):
        copy.start()

    def launch(n, carry):
        for side in (LOW, HIGH):
            lat_start(0, side, n)
        return carry

    lax.fori_loop(0, AHEAD, launch, 0)
    load_field.wait()

    def pack(position, carry):
        n = position // ROWS
        row = chunk_at(n) * ROWS + position % ROWS + 1
        for plane in range(depth):
            lev_face[0, LOW, position, pl.ds(plane, 1)] = even[plane, row, pl.ds(tall - 1, 1)]
            lev_face[0, HIGH, position, pl.ds(plane, 1)] = even[plane, row, pl.ds(0, 1)]
        return carry

    lax.fori_loop(0, width, pack, 0)
    for group in range(GROUPS):
        for copy in both(lev_copy, 0, group):
            copy.start()
    load_crowd.wait()

    for stage, (lead, there) in enumerate(zip(LEADS, (edge, corner))):

        @pl.when(there)
        def _(stage=stage, lead=lead):
            def begin(n, carry):
                send_on(0, stage, n)
                return carry

            lax.fori_loop(0, lead, begin, 0)

    place = lax.broadcasted_iota(jnp.int32, (8, 128), 0)

    def new_row(s, n, r):
        src, dst = bufs[s % 2], bufs[(s + 1) % 2]
        at = chunk_at(n) * ROWS + r
        row, position = at + 1, n * ROWS + r
        for plane in range(depth):
            for start, stop in ((0, 8), (8, 32), (32, 64), (64, tall - 8), (tall - 8, tall)):
                span = pl.ds(start, stop - start)
                middle = src[plane, row, span]
                if start == 0:
                    halo = lev_halo[s, LOW, position, pl.ds(plane, 1)]
                    lower = jnp.where(place == 0, halo, pltpu.roll(middle, 1, 0))
                else:
                    lower = src[plane, row, pl.ds(start - 1, stop - start)]
                if stop == tall:
                    halo = lev_halo[s, HIGH, position, pl.ds(plane, 1)]
                    upper = jnp.where(place == 7, halo, pltpu.roll(middle, 7, 0))
                else:
                    upper = src[plane, row, pl.ds(start + 1, stop - start)]
                around = lower + upper + src[plane, row - 1, span] + src[plane, row + 1, span]
                if plane == 0:
                    around += lat_halo[s % 2, LOW, at, span]
                else:
                    around += src[plane - 1, row, span]
                if plane == depth - 1:
                    around += lat_halo[s % 2, HIGH, at, span]
                else:
                    around += src[plane + 1, row, span]
                growth = 0.6 - 0.2 * (middle * crowd[plane, at, span])
                new = 0.1 * around + middle * growth
                if s == STEPS - 1:
                    crowd[plane, at, span] = new
                else:
                    dst[plane, row, span] = new
                if s < STEPS - 1:
                    if start == 0:
                        lev_face[s + 1, HIGH, position, pl.ds(plane, 1)] = new[0:1]
                    if stop == tall:
                        lev_face[s + 1, LOW, position, pl.ds(plane, 1)] = new[7:8]

    for s in range(STEPS):

        def chunk(n, carry, s=s):
            relays(s, n)
            for copy in both(lat_copy, s, n):
                copy.wait_recv()

            @pl.when(n + AHEAD < chunks)
            def _():
                if s > 0:
                    for copy in both(lat_copy, s - 1, n + AHEAD):
                        copy.wait_send()
                for side in (LOW, HIGH):
                    lat_start(s, side, n + AHEAD)

            if s < STEPS - 1:

                @pl.when(n + AHEAD >= chunks)
                def _():
                    for copy in both(lat_copy, s, n + AHEAD - chunks):
                        copy.wait_send()
                    for side in (LOW, HIGH):
                        lat_start(s + 1, side, n + AHEAD - chunks)

            @pl.when(n == 0)
            def _():
                if s > 0:
                    for copy in both(lev_copy, s, GROUPS - 1):
                        copy.start()
                    for copy in both(lon_copy, s - 1):
                        copy.wait_send()
                for copy in both(lon_copy, s):
                    copy.wait_recv()

            if s < STEPS - 1:

                @pl.when(n == 2)
                def _():
                    for copy in both(lon_copy, s + 1):
                        copy.start()

            @pl.when(n % each == 0)
            def _():
                for copy in both(lev_copy, s, n // each):
                    copy.wait_recv()
                if s < STEPS - 1:

                    @pl.when(n > 0)
                    def _():
                        for copy in both(lev_copy, s + 1, n // each - 1):
                            copy.start()

            def row(r, inner):
                new_row(s, n, r)
                return inner

            return lax.fori_loop(0, ROWS, row, carry)

        lax.fori_loop(0, chunks, chunk, 0)

    def drain(n, carry):
        for copy in both(lat_copy, STEPS - 1, n):
            copy.wait_send()
        return carry

    for copy in both(lon_copy, STEPS - 1):
        copy.wait_send()
    for t in range(STEPS):
        for group in range(GROUPS):
            for copy in both(lev_copy, t, group):
                copy.wait_send()
    lax.fori_loop(0, chunks, drain, 0)

    for stage, there in enumerate((edge, corner)):

        @pl.when(there)
        def _(stage=stage):
            def settle(n, carry):
                relay_copy(STEPS - 1, stage, n, True).wait_send()
                return carry

            lax.fori_loop(chunks - SETTLE, DIRECT, settle, 0)


def local(field, crowding):
    depth, width, tall, lanes = field.shape
    chunks = width // ROWS
    padded = (depth, width + 2, tall, lanes)
    faces = (STEPS, 2, width, depth, lanes)
    dma = pltpu.SemaphoreType.DMA
    return pl.pallas_call(
        kernel,
        out_shape=pltpu.VMEM(field.shape, field.dtype),
        in_specs=[pl.BlockSpec(memory_space=pl.ANY)] * 2,
        out_specs=pl.BlockSpec(memory_space=pltpu.VMEM),
        scratch_shapes=[
            pltpu.VMEM(padded, jnp.float32),
            pltpu.VMEM(padded, jnp.float32),
            pltpu.VMEM((2, 2, width, tall, lanes), jnp.float32),
            pltpu.VMEM(faces, jnp.float32),
            pltpu.VMEM(faces, jnp.float32),
            pltpu.VMEM((2, width, tall, lanes), jnp.float32),
            dma((2,)),
            dma((2, chunks)),
            dma((2, 2, chunks)),
            dma((STEPS, 2)),
            dma((STEPS, 2)),
            dma((STEPS, 2, GROUPS)),
            dma((STEPS, 2, GROUPS)),
            dma((2, chunks)),
            dma((2, chunks)),
        ],
        compiler_params=pltpu.CompilerParams(
            collective_id=0, has_side_effects=True, vmem_limit_bytes=46 * 1024 * 1024
        ),
        name="march",
    )(field, crowding)


def solution(mesh):
    spec = P("lat", "lon", "lev", None)
    return jax.shard_map(
        local, mesh=mesh, in_specs=(spec, spec), out_specs=spec, check_vma=False
    )
```

```python
import functools

import jax
import jax.numpy as jnp
from jax import lax
from jax.experimental import pallas as pl
from jax.experimental.pallas import tpu as pltpu
from jax.sharding import PartitionSpec as P

STEPS = 3
ROWS = 2
AHEAD = 10
LEADS = (4, 2)
SETTLE = 6
DIRECT = 32
PASS = 10
GROUPS = 4
LOW, HIGH = 0, 1


def kernel(
    field, crowding, crowd,
    even, odd, lat_halo, lev_face, lev_halo, relay, lev_pass,
    load_sem, lat_send, lat_recv, lon_send, lon_recv, lev_send, lev_recv,
    relay_send, relay_recv, pass_send, pass_recv,
):
    depth, width, tall, _ = field.shape
    chunks = width // ROWS
    each = chunks // GROUPS
    bufs = (even, odd)

    def beside(axis, step):
        size = lax.axis_size(axis)
        return {axis: lax.rem(lax.axis_index(axis) + step + size, size)}

    lat_at = (beside("lat", -1), beside("lat", 1))
    lon_at = (beside("lon", -1), beside("lon", 1))
    lev_at = (beside("lev", -1), beside("lev", 1))

    lat = lax.axis_index("lat")
    x, y = lat % 4, (lat // 4) % 2
    first, last = x == 0, x == 3
    edge = first | last
    corner = (first & (y == 0)) | (last & (y == 1))
    mine = jnp.where(first, LOW, HIGH)
    across = {"lat": jnp.where(first, lat + 3, jnp.where(last, lat - 3, lat))}
    turned = {"lat": jnp.where(y == 0, lat + 4, lat - 4)}
    lifted = {"lat": lax.rem(lat + 8, 16)}

    inside = lat + jnp.where(x % 2 == 0, 1, -1)
    aslant = {"lat": inside, **beside("lev", 1)}
    inward = {"lat": inside}

    def chunk_at(n):
        return jnp.where(n == 0, 0, jnp.where(n == 1, chunks - 1, n - 1))

    load_field = pltpu.make_async_copy(field, even.at[:, pl.ds(1, width)], load_sem.at[0])
    load_crowd = pltpu.make_async_copy(crowding, crowd, load_sem.at[1])

    def lat_copy(t, side, n):
        plane = depth - 1 if side == LOW else 0
        rows = chunk_at(n) * ROWS
        if t == 0:
            src = field.at[plane, pl.ds(rows, ROWS)]
        else:
            src = bufs[t % 2].at[plane, pl.ds(rows + 1, ROWS)]
        return pltpu.make_async_remote_copy(
            src_ref=src,
            dst_ref=lat_halo.at[t % 2, side, pl.ds(rows, ROWS)],
            send_sem=lat_send.at[side, n],
            recv_sem=lat_recv.at[t % 2, side, n],
            device_id=lat_at[1 - side],
            device_id_type=pl.DeviceIdType.MESH,
        )

    def lat_start(t, side, n):
        plain = lat_copy(t, side, n)
        leaves = last if side == LOW else first
        if t == STEPS - 1:
            leaves = leaves & (n < DIRECT)

        @pl.when(leaves)
        def _():
            pltpu.make_async_remote_copy(
                src_ref=plain.src_ref,
                dst_ref=relay.at[0, pl.ds(chunk_at(n) * ROWS, ROWS)],
                send_sem=lat_send.at[side, n],
                recv_sem=relay_recv.at[0, n],
                device_id=across,
                device_id_type=pl.DeviceIdType.MESH,
            ).start()

        @pl.when(jnp.logical_not(leaves))
        def _():
            plain.start()

    def relay_copy(t, stage, n, arrives):
        rows = pl.ds(chunk_at(n) * ROWS, ROWS)
        return pltpu.make_async_remote_copy(
            src_ref=relay.at[stage, rows],
            dst_ref=lat_halo.at[t % 2, mine, rows] if arrives else relay.at[1, rows],
            send_sem=relay_send.at[stage, n],
            recv_sem=lat_recv.at[t % 2, mine, n] if arrives else relay_recv.at[1, n],
            device_id=lifted if stage else turned,
            device_id_type=pl.DeviceIdType.MESH,
        )

    def relay_landed(stage, n):
        rows = pl.ds(chunk_at(n) * ROWS, ROWS)
        pltpu.make_async_remote_copy(
            src_ref=relay.at[stage, rows],
            dst_ref=relay.at[stage, rows],
            send_sem=relay_send.at[stage, n],
            recv_sem=relay_recv.at[stage, n],
            device_id=lifted,
            device_id_type=pl.DeviceIdType.MESH,
        ).wait_recv()

    def send_on(t, stage, n):
        relay_landed(stage, n)
        if stage == 1:
            relay_copy(t, stage, n, True).start()
            return

        @pl.when(corner)
        def _():
            relay_copy(t, stage, n, True).start()

        @pl.when(jnp.logical_not(corner))
        def _():
            relay_copy(t, stage, n, False).start()

    def relays(s, n):
        for stage, (lead, there) in enumerate(zip(LEADS, (edge, corner))):
            ahead = n + lead
            here = there & (ahead < (DIRECT if s == STEPS - 1 else chunks))

            @pl.when(here)
            def _():
                send_on(s, stage, ahead)

            if s < STEPS - 1:
                end = DIRECT if s + 1 == STEPS - 1 else chunks

                @pl.when(there & (ahead >= chunks) & (ahead - chunks < end))
                def _():
                    send_on(s + 1, stage, ahead - chunks)

            left = n - SETTLE

            @pl.when(there & (left >= 0) & (left < (DIRECT if s == STEPS - 1 else chunks)))
            def _():
                relay_copy(s, stage, left, True).wait_send()

            if s > 0:

                @pl.when(there & (left < 0))
                def _():
                    relay_copy(s - 1, stage, left + chunks, True).wait_send()

    def lon_copy(t, side):
        row = width - 1 if side == LOW else 0
        src = field.at[:, row] if t == 0 else bufs[t % 2].at[:, row + 1]
        return pltpu.make_async_remote_copy(
            src_ref=src,
            dst_ref=bufs[t % 2].at[:, 0 if side == LOW else width + 1],
            send_sem=lon_send.at[t, side],
            recv_sem=lon_recv.at[t, side],
            device_id=lon_at[1 - side],
            device_id_type=pl.DeviceIdType.MESH,
        )

    def lev_copy(t, side, group):
        rows = pl.ds(group * (each * ROWS), each * ROWS)
        return pltpu.make_async_remote_copy(
            src_ref=lev_face.at[t, side, rows],
            dst_ref=lev_halo.at[t, side, rows],
            send_sem=lev_send.at[t, side, group],
            recv_sem=lev_recv.at[t, side, group],
            device_id=lev_at[1 - side],
            device_id_type=pl.DeviceIdType.MESH,
        )

    def lev_start(t, group):
        plain = lev_copy(t, HIGH, group)
        lev_copy(t, LOW, group).start()
        if t == 0:
            plain.start()
            return

        @pl.when(edge)
        def _():
            pltpu.make_async_remote_copy(
                src_ref=plain.src_ref,
                dst_ref=lev_pass.at[t, pl.ds(group * (each * ROWS), each * ROWS)],
                send_sem=lev_send.at[t, HIGH, group],
                recv_sem=pass_recv.at[t, group],
                device_id=aslant,
                device_id_type=pl.DeviceIdType.MESH,
            ).start()

        @pl.when(jnp.logical_not(edge))
        def _():
            plain.start()

    def pass_copy(t, group, landing=False):
        rows = pl.ds(group * (each * ROWS), each * ROWS)
        return pltpu.make_async_remote_copy(
            src_ref=lev_pass.at[t, rows],
            dst_ref=lev_pass.at[t, rows] if landing else lev_halo.at[t, HIGH, rows],
            send_sem=pass_send.at[t, group],
            recv_sem=pass_recv.at[t, group] if landing else lev_recv.at[t, HIGH, group],
            device_id=inward,
            device_id_type=pl.DeviceIdType.MESH,
        )

    def pass_on(s, n):
        for t, since in ((s + 1, n - each - PASS), (s, n + chunks - each - PASS)):
            if 0 < t < STEPS:
                here = (since >= 0) & (since % each == 0) & (since < chunks)

                @pl.when(here & jnp.logical_not(edge))
                def _():
                    pass_copy(t, since // each, True).wait_recv()
                    pass_copy(t, since // each).start()

    def both(copy, *where):
        return [copy(*(where[:1] + (side,) + where[1:])) for side in (LOW, HIGH)]

    load_field.start()
    load_crowd.start()
    barrier = pltpu.get_barrier_semaphore()

    def greet(partners):
        for partner in partners:
            pl.semaphore_signal(
                barrier, inc=1, device_id=partner, device_id_type=pl.DeviceIdType.MESH
            )

    greet((*lat_at, *lon_at, lev_at[0], aslant))

    @pl.when(edge)
    def _():
        greet((across, turned, lifted))

    pl.semaphore_wait(barrier, jnp.where(edge, 9, 6))

    for copy in both(lon_copy, 0):
        copy.start()

    def launch(n, carry):
        for side in (LOW, HIGH):
            lat_start(0, side, n)
        return carry

    lax.fori_loop(0, AHEAD, launch, 0)
    load_field.wait()

    def pack(position, carry):
        n = position // ROWS
        row = chunk_at(n) * ROWS + position % ROWS + 1
        for plane in range(depth):
            lev_face[0, LOW, position, pl.ds(plane, 1)] = even[plane, row, pl.ds(tall - 1, 1)]
            lev_face[0, HIGH, position, pl.ds(plane, 1)] = even[plane, row, pl.ds(0, 1)]
        return carry

    lax.fori_loop(0, width, pack, 0)
    for group in range(GROUPS):
        for copy in both(lev_copy, 0, group):
            copy.start()
    load_crowd.wait()

    for stage, (lead, there) in enumerate(zip(LEADS, (edge, corner))):

        @pl.when(there)
        def _(stage=stage, lead=lead):
            def begin(n, carry):
                send_on(0, stage, n)
                return carry

            lax.fori_loop(0, lead, begin, 0)

    place = lax.broadcasted_iota(jnp.int32, (8, 128), 0)

    def new_row(s, n, r):
        src, dst = bufs[s % 2], bufs[(s + 1) % 2]
        at = chunk_at(n) * ROWS + r
        row, position = at + 1, n * ROWS + r
        for plane in range(depth):
            for start, stop in ((0, 8), (8, 32), (32, 64), (64, tall - 8), (tall - 8, tall)):
                span = pl.ds(start, stop - start)
                middle = src[plane, row, span]
                if start == 0:
                    halo = lev_halo[s, LOW, position, pl.ds(plane, 1)]
                    lower = jnp.where(place == 0, halo, pltpu.roll(middle, 1, 0))
                else:
                    lower = src[plane, row, pl.ds(start - 1, stop - start)]
                if stop == tall:
                    halo = lev_halo[s, HIGH, position, pl.ds(plane, 1)]
                    upper = jnp.where(place == 7, halo, pltpu.roll(middle, 7, 0))
                else:
                    upper = src[plane, row, pl.ds(start + 1, stop - start)]
                around = lower + upper + src[plane, row - 1, span] + src[plane, row + 1, span]
                if plane == 0:
                    around += lat_halo[s % 2, LOW, at, span]
                else:
                    around += src[plane - 1, row, span]
                if plane == depth - 1:
                    around += lat_halo[s % 2, HIGH, at, span]
                else:
                    around += src[plane + 1, row, span]
                growth = 0.6 - 0.2 * (middle * crowd[plane, at, span])
                new = 0.1 * around + middle * growth
                if s == STEPS - 1:
                    crowd[plane, at, span] = new
                else:
                    dst[plane, row, span] = new
                if s < STEPS - 1:
                    if start == 0:
                        lev_face[s + 1, HIGH, position, pl.ds(plane, 1)] = new[0:1]
                    if stop == tall:
                        lev_face[s + 1, LOW, position, pl.ds(plane, 1)] = new[7:8]

    for s in range(STEPS):

        def chunk(n, carry, s=s):
            relays(s, n)
            pass_on(s, n)
            for copy in both(lat_copy, s, n):
                copy.wait_recv()

            @pl.when(n + AHEAD < chunks)
            def _():
                if s > 0:
                    for copy in both(lat_copy, s - 1, n + AHEAD):
                        copy.wait_send()
                for side in (LOW, HIGH):
                    lat_start(s, side, n + AHEAD)

            if s < STEPS - 1:

                @pl.when(n + AHEAD >= chunks)
                def _():
                    for copy in both(lat_copy, s, n + AHEAD - chunks):
                        copy.wait_send()
                    for side in (LOW, HIGH):
                        lat_start(s + 1, side, n + AHEAD - chunks)

            @pl.when(n == 0)
            def _():
                if s > 0:
                    lev_start(s, GROUPS - 1)
                    for copy in both(lon_copy, s - 1):
                        copy.wait_send()
                for copy in both(lon_copy, s):
                    copy.wait_recv()

            if s < STEPS - 1:

                @pl.when(n == 2)
                def _():
                    for copy in both(lon_copy, s + 1):
                        copy.start()

            @pl.when(n % each == 0)
            def _():
                for copy in both(lev_copy, s, n // each):
                    copy.wait_recv()
                if s < STEPS - 1:

                    @pl.when(n > 0)
                    def _():
                        lev_start(s + 1, n // each - 1)

            def row(r, inner):
                new_row(s, n, r)
                return inner

            return lax.fori_loop(0, ROWS, row, carry)

        lax.fori_loop(0, chunks, chunk, 0)

    def drain(n, carry):
        for copy in both(lat_copy, STEPS - 1, n):
            copy.wait_send()
        return carry

    for copy in both(lon_copy, STEPS - 1):
        copy.wait_send()
    for t in range(STEPS):
        for group in range(GROUPS):
            for copy in both(lev_copy, t, group):
                copy.wait_send()
    lax.fori_loop(0, chunks, drain, 0)

    @pl.when(jnp.logical_not(edge))
    def _():
        for t in range(1, STEPS):
            for group in range(GROUPS):
                pass_copy(t, group).wait_send()

    for stage, there in enumerate((edge, corner)):

        @pl.when(there)
        def _(stage=stage):
            def settle(n, carry):
                relay_copy(STEPS - 1, stage, n, True).wait_send()
                return carry

            lax.fori_loop(chunks - SETTLE, DIRECT, settle, 0)


def local(field, crowding):
    depth, width, tall, lanes = field.shape
    chunks = width // ROWS
    padded = (depth, width + 2, tall, lanes)
    faces = (STEPS, 2, width, depth, lanes)
    dma = pltpu.SemaphoreType.DMA
    return pl.pallas_call(
        kernel,
        out_shape=pltpu.VMEM(field.shape, field.dtype),
        in_specs=[pl.BlockSpec(memory_space=pl.ANY)] * 2,
        out_specs=pl.BlockSpec(memory_space=pltpu.VMEM),
        scratch_shapes=[
            pltpu.VMEM(padded, jnp.float32),
            pltpu.VMEM(padded, jnp.float32),
            pltpu.VMEM((2, 2, width, tall, lanes), jnp.float32),
            pltpu.VMEM(faces, jnp.float32),
            pltpu.VMEM(faces, jnp.float32),
            pltpu.VMEM((2, width, tall, lanes), jnp.float32),
            pltpu.VMEM((STEPS, width, depth, lanes), jnp.float32),
            dma((2,)),
            dma((2, chunks)),
            dma((2, 2, chunks)),
            dma((STEPS, 2)),
            dma((STEPS, 2)),
            dma((STEPS, 2, GROUPS)),
            dma((STEPS, 2, GROUPS)),
            dma((2, chunks)),
            dma((2, chunks)),
            dma((STEPS, GROUPS)),
            dma((STEPS, GROUPS)),
        ],
        compiler_params=pltpu.CompilerParams(
            collective_id=0, has_side_effects=True, vmem_limit_bytes=46 * 1024 * 1024
        ),
        name="march",
    )(field, crowding)


def solution(mesh):
    spec = P("lat", "lon", "lev", None)
    return jax.shard_map(
        local, mesh=mesh, in_specs=(spec, spec), out_specs=spec, check_vma=False
    )
```

```python
import functools

import jax
import jax.numpy as jnp
from jax import lax
from jax.experimental import pallas as pl
from jax.experimental.pallas import tpu as pltpu
from jax.sharding import PartitionSpec as P

STEPS = 3
ROWS = 2
AHEAD = 10
LEADS = (4, 2)
SETTLE = 6
PASS = 10
GROUPS = 4
LOW, HIGH = 0, 1


def kernel(
    field, crowding, crowd,
    even, odd, lat_halo, lev_face, lev_halo, relay, lev_pass,
    load_sem, lat_send, lat_recv, lon_send, lon_recv, lev_send, lev_recv,
    relay_send, relay_recv, pass_send, pass_recv,
):
    depth, width, tall, _ = field.shape
    chunks = width // ROWS
    each = chunks // GROUPS
    bufs = (even, odd)

    def beside(axis, step):
        size = lax.axis_size(axis)
        return {axis: lax.rem(lax.axis_index(axis) + step + size, size)}

    lat_at = (beside("lat", -1), beside("lat", 1))
    lon_at = (beside("lon", -1), beside("lon", 1))
    lev_at = (beside("lev", -1), beside("lev", 1))

    lat = lax.axis_index("lat")
    x, y = lat % 4, (lat // 4) % 2
    first, last = x == 0, x == 3
    edge = first | last
    corner = (first & (y == 0)) | (last & (y == 1))
    mine = jnp.where(first, LOW, HIGH)
    across = {"lat": jnp.where(first, lat + 3, jnp.where(last, lat - 3, lat))}
    turned = {"lat": jnp.where(y == 0, lat + 4, lat - 4)}
    lifted = {"lat": lax.rem(lat + 8, 16)}
    onward = {"lat": jnp.where(corner, lifted["lat"], turned["lat"])}

    def held(stage, n):
        return edge if stage == 0 else edge & (n % 2 == jnp.where(corner, 0, 1))


    inside = lat + jnp.where(x % 2 == 0, 1, -1)
    aslant = {"lat": inside, **beside("lev", 1)}
    inward = {"lat": inside}

    def chunk_at(n):
        return jnp.where(n == 0, 0, jnp.where(n == 1, chunks - 1, n - 1))

    load_field = pltpu.make_async_copy(field, even.at[:, pl.ds(1, width)], load_sem.at[0])
    load_crowd = pltpu.make_async_copy(crowding, crowd, load_sem.at[1])

    def lat_copy(t, side, n):
        plane = depth - 1 if side == LOW else 0
        rows = chunk_at(n) * ROWS
        if t == 0:
            src = field.at[plane, pl.ds(rows, ROWS)]
        else:
            src = bufs[t % 2].at[plane, pl.ds(rows + 1, ROWS)]
        return pltpu.make_async_remote_copy(
            src_ref=src,
            dst_ref=lat_halo.at[t % 2, side, pl.ds(rows, ROWS)],
            send_sem=lat_send.at[side, n],
            recv_sem=lat_recv.at[t % 2, side, n],
            device_id=lat_at[1 - side],
            device_id_type=pl.DeviceIdType.MESH,
        )

    def lat_start(t, side, n):
        plain = lat_copy(t, side, n)
        leaves = last if side == LOW else first
        @pl.when(leaves)
        def _():
            pltpu.make_async_remote_copy(
                src_ref=plain.src_ref,
                dst_ref=relay.at[0, pl.ds(chunk_at(n) * ROWS, ROWS)],
                send_sem=lat_send.at[side, n],
                recv_sem=relay_recv.at[0, n],
                device_id=across,
                device_id_type=pl.DeviceIdType.MESH,
            ).start()

        @pl.when(jnp.logical_not(leaves))
        def _():
            plain.start()

    def relay_copy(t, stage, n, arrives, target=None):
        rows = pl.ds(chunk_at(n) * ROWS, ROWS)
        return pltpu.make_async_remote_copy(
            src_ref=relay.at[stage, rows],
            dst_ref=lat_halo.at[t % 2, mine, rows] if arrives else relay.at[1, rows],
            send_sem=relay_send.at[stage, n],
            recv_sem=lat_recv.at[t % 2, mine, n] if arrives else relay_recv.at[1, n],
            device_id=target or (onward if stage else turned),
            device_id_type=pl.DeviceIdType.MESH,
        )

    def relay_landed(stage, n):
        rows = pl.ds(chunk_at(n) * ROWS, ROWS)
        pltpu.make_async_remote_copy(
            src_ref=relay.at[stage, rows],
            dst_ref=relay.at[stage, rows],
            send_sem=relay_send.at[stage, n],
            recv_sem=relay_recv.at[stage, n],
            device_id=lifted,
            device_id_type=pl.DeviceIdType.MESH,
        ).wait_recv()

    def send_on(t, stage, n):
        relay_landed(stage, n)
        if stage == 1:
            relay_copy(t, stage, n, True).start()
            return

        @pl.when(corner)
        def _():
            relay_copy(t, stage, n, True).start()

        @pl.when(jnp.logical_not(corner) & (n % 2 == 0))
        def _():
            relay_copy(t, stage, n, False, turned).start()

        @pl.when(jnp.logical_not(corner) & (n % 2 == 1))
        def _():
            relay_copy(t, stage, n, False, lifted).start()

    def relays(s, n):
        for stage, lead in enumerate(LEADS):
            ahead = n + lead
            there = held(stage, ahead)
            here = there & (ahead < chunks)

            @pl.when(here)
            def _():
                send_on(s, stage, ahead)

            if s < STEPS - 1:
                @pl.when(there & (ahead >= chunks))
                def _():
                    send_on(s + 1, stage, ahead - chunks)

            left = n - SETTLE
            there = held(stage, left + chunks)

            @pl.when(there & (left >= 0))
            def _():
                relay_copy(s, stage, left, True).wait_send()

            if s > 0:

                @pl.when(there & (left < 0))
                def _():
                    relay_copy(s - 1, stage, left + chunks, True).wait_send()

    def lon_copy(t, side):
        row = width - 1 if side == LOW else 0
        src = field.at[:, row] if t == 0 else bufs[t % 2].at[:, row + 1]
        return pltpu.make_async_remote_copy(
            src_ref=src,
            dst_ref=bufs[t % 2].at[:, 0 if side == LOW else width + 1],
            send_sem=lon_send.at[t, side],
            recv_sem=lon_recv.at[t, side],
            device_id=lon_at[1 - side],
            device_id_type=pl.DeviceIdType.MESH,
        )

    def lev_copy(t, side, group):
        rows = pl.ds(group * (each * ROWS), each * ROWS)
        return pltpu.make_async_remote_copy(
            src_ref=lev_face.at[t, side, rows],
            dst_ref=lev_halo.at[t, side, rows],
            send_sem=lev_send.at[t, side, group],
            recv_sem=lev_recv.at[t, side, group],
            device_id=lev_at[1 - side],
            device_id_type=pl.DeviceIdType.MESH,
        )

    def lev_start(t, group):
        plain = lev_copy(t, HIGH, group)
        lev_copy(t, LOW, group).start()
        if t == 0:
            plain.start()
            return

        @pl.when(edge)
        def _():
            pltpu.make_async_remote_copy(
                src_ref=plain.src_ref,
                dst_ref=lev_pass.at[t, pl.ds(group * (each * ROWS), each * ROWS)],
                send_sem=lev_send.at[t, HIGH, group],
                recv_sem=pass_recv.at[t, group],
                device_id=aslant,
                device_id_type=pl.DeviceIdType.MESH,
            ).start()

        @pl.when(jnp.logical_not(edge))
        def _():
            plain.start()

    def pass_copy(t, group, landing=False):
        rows = pl.ds(group * (each * ROWS), each * ROWS)
        return pltpu.make_async_remote_copy(
            src_ref=lev_pass.at[t, rows],
            dst_ref=lev_pass.at[t, rows] if landing else lev_halo.at[t, HIGH, rows],
            send_sem=pass_send.at[t, group],
            recv_sem=pass_recv.at[t, group] if landing else lev_recv.at[t, HIGH, group],
            device_id=inward,
            device_id_type=pl.DeviceIdType.MESH,
        )

    def pass_on(s, n):
        for t, since in ((s + 1, n - each - PASS), (s, n + chunks - each - PASS)):
            if 0 < t < STEPS:
                here = (since >= 0) & (since % each == 0) & (since < chunks)

                @pl.when(here & jnp.logical_not(edge))
                def _():
                    pass_copy(t, since // each, True).wait_recv()
                    pass_copy(t, since // each).start()

    def both(copy, *where):
        return [copy(*(where[:1] + (side,) + where[1:])) for side in (LOW, HIGH)]

    load_field.start()
    load_crowd.start()
    barrier = pltpu.get_barrier_semaphore()

    def greet(partners):
        for partner in partners:
            pl.semaphore_signal(
                barrier, inc=1, device_id=partner, device_id_type=pl.DeviceIdType.MESH
            )

    greet((*lat_at, *lon_at, lev_at[0], aslant))

    @pl.when(edge)
    def _():
        greet((across, turned, lifted))

    pl.semaphore_wait(barrier, jnp.where(edge, 9, 6))

    for copy in both(lon_copy, 0):
        copy.start()

    def launch(n, carry):
        for side in (LOW, HIGH):
            lat_start(0, side, n)
        return carry

    lax.fori_loop(0, AHEAD, launch, 0)
    load_field.wait()

    def pack(position, carry):
        n = position // ROWS
        row = chunk_at(n) * ROWS + position % ROWS + 1
        for plane in range(depth):
            lev_face[0, LOW, position, pl.ds(plane, 1)] = even[plane, row, pl.ds(tall - 1, 1)]
            lev_face[0, HIGH, position, pl.ds(plane, 1)] = even[plane, row, pl.ds(0, 1)]
        return carry

    lax.fori_loop(0, width, pack, 0)
    for group in range(GROUPS):
        for copy in both(lev_copy, 0, group):
            copy.start()
    load_crowd.wait()

    for stage, lead in enumerate(LEADS):

        def begin(n, carry, stage=stage):
            @pl.when(held(stage, n))
            def _():
                send_on(0, stage, n)

            return carry

        lax.fori_loop(0, lead, begin, 0)

    place = lax.broadcasted_iota(jnp.int32, (8, 128), 0)

    def new_row(s, n, r):
        src, dst = bufs[s % 2], bufs[(s + 1) % 2]
        at = chunk_at(n) * ROWS + r
        row, position = at + 1, n * ROWS + r
        for plane in range(depth):
            for start, stop in ((0, 8), (8, 32), (32, 64), (64, tall - 8), (tall - 8, tall)):
                span = pl.ds(start, stop - start)
                middle = src[plane, row, span]
                if start == 0:
                    halo = lev_halo[s, LOW, position, pl.ds(plane, 1)]
                    lower = jnp.where(place == 0, halo, pltpu.roll(middle, 1, 0))
                else:
                    lower = src[plane, row, pl.ds(start - 1, stop - start)]
                if stop == tall:
                    halo = lev_halo[s, HIGH, position, pl.ds(plane, 1)]
                    upper = jnp.where(place == 7, halo, pltpu.roll(middle, 7, 0))
                else:
                    upper = src[plane, row, pl.ds(start + 1, stop - start)]
                around = lower + upper + src[plane, row - 1, span] + src[plane, row + 1, span]
                if plane == 0:
                    around += lat_halo[s % 2, LOW, at, span]
                else:
                    around += src[plane - 1, row, span]
                if plane == depth - 1:
                    around += lat_halo[s % 2, HIGH, at, span]
                else:
                    around += src[plane + 1, row, span]
                growth = 0.6 - 0.2 * (middle * crowd[plane, at, span])
                new = 0.1 * around + middle * growth
                if s == STEPS - 1:
                    crowd[plane, at, span] = new
                else:
                    dst[plane, row, span] = new
                if s < STEPS - 1:
                    if start == 0:
                        lev_face[s + 1, HIGH, position, pl.ds(plane, 1)] = new[0:1]
                    if stop == tall:
                        lev_face[s + 1, LOW, position, pl.ds(plane, 1)] = new[7:8]

    for s in range(STEPS):

        def chunk(n, carry, s=s):
            relays(s, n)
            pass_on(s, n)
            for copy in both(lat_copy, s, n):
                copy.wait_recv()

            @pl.when(n + AHEAD < chunks)
            def _():
                if s > 0:
                    for copy in both(lat_copy, s - 1, n + AHEAD):
                        copy.wait_send()
                for side in (LOW, HIGH):
                    lat_start(s, side, n + AHEAD)

            if s < STEPS - 1:

                @pl.when(n + AHEAD >= chunks)
                def _():
                    for copy in both(lat_copy, s, n + AHEAD - chunks):
                        copy.wait_send()
                    for side in (LOW, HIGH):
                        lat_start(s + 1, side, n + AHEAD - chunks)

            @pl.when(n == 0)
            def _():
                if s > 0:
                    lev_start(s, GROUPS - 1)
                    for copy in both(lon_copy, s - 1):
                        copy.wait_send()
                for copy in both(lon_copy, s):
                    copy.wait_recv()

            if s < STEPS - 1:

                @pl.when(n == 2)
                def _():
                    for copy in both(lon_copy, s + 1):
                        copy.start()

            @pl.when(n % each == 0)
            def _():
                for copy in both(lev_copy, s, n // each):
                    copy.wait_recv()
                if s < STEPS - 1:

                    @pl.when(n > 0)
                    def _():
                        lev_start(s + 1, n // each - 1)

            def row(r, inner):
                new_row(s, n, r)
                return inner

            return lax.fori_loop(0, ROWS, row, carry)

        lax.fori_loop(0, chunks, chunk, 0)

    def drain(n, carry):
        for copy in both(lat_copy, STEPS - 1, n):
            copy.wait_send()
        return carry

    for copy in both(lon_copy, STEPS - 1):
        copy.wait_send()
    for t in range(STEPS):
        for group in range(GROUPS):
            for copy in both(lev_copy, t, group):
                copy.wait_send()
    lax.fori_loop(0, chunks, drain, 0)

    @pl.when(jnp.logical_not(edge))
    def _():
        for t in range(1, STEPS):
            for group in range(GROUPS):
                pass_copy(t, group).wait_send()

    for stage in (0, 1):

        def settle(n, carry, stage=stage):
            @pl.when(held(stage, n))
            def _():
                relay_copy(STEPS - 1, stage, n, True).wait_send()

            return carry

        lax.fori_loop(chunks - SETTLE, chunks, settle, 0)


def local(field, crowding):
    depth, width, tall, lanes = field.shape
    chunks = width // ROWS
    padded = (depth, width + 2, tall, lanes)
    faces = (STEPS, 2, width, depth, lanes)
    dma = pltpu.SemaphoreType.DMA
    return pl.pallas_call(
        kernel,
        out_shape=pltpu.VMEM(field.shape, field.dtype),
        in_specs=[pl.BlockSpec(memory_space=pl.ANY)] * 2,
        out_specs=pl.BlockSpec(memory_space=pltpu.VMEM),
        scratch_shapes=[
            pltpu.VMEM(padded, jnp.float32),
            pltpu.VMEM(padded, jnp.float32),
            pltpu.VMEM((2, 2, width, tall, lanes), jnp.float32),
            pltpu.VMEM(faces, jnp.float32),
            pltpu.VMEM(faces, jnp.float32),
            pltpu.VMEM((2, width, tall, lanes), jnp.float32),
            pltpu.VMEM((STEPS, width, depth, lanes), jnp.float32),
            dma((2,)),
            dma((2, chunks)),
            dma((2, 2, chunks)),
            dma((STEPS, 2)),
            dma((STEPS, 2)),
            dma((STEPS, 2, GROUPS)),
            dma((STEPS, 2, GROUPS)),
            dma((2, chunks)),
            dma((2, chunks)),
            dma((STEPS, GROUPS)),
            dma((STEPS, GROUPS)),
        ],
        compiler_params=pltpu.CompilerParams(
            collective_id=0, has_side_effects=True, vmem_limit_bytes=46 * 1024 * 1024
        ),
        name="march",
    )(field, crowding)


def solution(mesh):
    spec = P("lat", "lon", "lev", None)
    return jax.shard_map(
        local, mesh=mesh, in_specs=(spec, spec), out_specs=spec, check_vma=False
    )
```

```python
import functools

import jax
import jax.numpy as jnp
from jax import lax
from jax.experimental import pallas as pl
from jax.experimental.pallas import tpu as pltpu
from jax.sharding import PartitionSpec as P

STEPS = 3
ROWS = 2
AHEAD = 10
LEADS = (4, 2)
SETTLE = 6
PASS = 10
GROUPS = 8
LOW, HIGH = 0, 1


def kernel(
    field, crowding, crowd,
    even, odd, lat_halo, lev_face, lev_halo, relay, lev_pass,
    load_sem, lat_send, lat_recv, lon_send, lon_recv, lev_send, lev_recv,
    relay_send, relay_recv, pass_send, pass_recv,
):
    depth, width, tall, _ = field.shape
    chunks = width // ROWS
    each = chunks // GROUPS
    bufs = (even, odd)

    def beside(axis, step):
        size = lax.axis_size(axis)
        return {axis: lax.rem(lax.axis_index(axis) + step + size, size)}

    lat_at = (beside("lat", -1), beside("lat", 1))
    lon_at = (beside("lon", -1), beside("lon", 1))
    lev_at = (beside("lev", -1), beside("lev", 1))

    lat = lax.axis_index("lat")
    x, y = lat % 4, (lat // 4) % 2
    first, last = x == 0, x == 3
    edge = first | last
    corner = (first & (y == 0)) | (last & (y == 1))
    mine = jnp.where(first, LOW, HIGH)
    across = {"lat": jnp.where(first, lat + 3, jnp.where(last, lat - 3, lat))}
    turned = {"lat": jnp.where(y == 0, lat + 4, lat - 4)}
    lifted = {"lat": lax.rem(lat + 8, 16)}
    onward = {"lat": jnp.where(corner, lifted["lat"], turned["lat"])}

    def held(stage, n):
        return edge if stage == 0 else edge & (n % 2 == jnp.where(corner, 0, 1))


    inside = lat + jnp.where(x % 2 == 0, 1, -1)
    aslant = {"lat": inside, **beside("lev", 1)}
    inward = {"lat": inside}

    def chunk_at(n):
        return jnp.where(n == 0, 0, jnp.where(n == 1, chunks - 1, n - 1))

    load_field = pltpu.make_async_copy(field, even.at[:, pl.ds(1, width)], load_sem.at[0])
    load_crowd = pltpu.make_async_copy(crowding, crowd, load_sem.at[1])

    def lat_copy(t, side, n):
        plane = depth - 1 if side == LOW else 0
        rows = chunk_at(n) * ROWS
        if t == 0:
            src = field.at[plane, pl.ds(rows, ROWS)]
        else:
            src = bufs[t % 2].at[plane, pl.ds(rows + 1, ROWS)]
        return pltpu.make_async_remote_copy(
            src_ref=src,
            dst_ref=lat_halo.at[t % 2, side, pl.ds(rows, ROWS)],
            send_sem=lat_send.at[side, n],
            recv_sem=lat_recv.at[t % 2, side, n],
            device_id=lat_at[1 - side],
            device_id_type=pl.DeviceIdType.MESH,
        )

    def lat_start(t, side, n):
        plain = lat_copy(t, side, n)
        leaves = last if side == LOW else first
        @pl.when(leaves)
        def _():
            pltpu.make_async_remote_copy(
                src_ref=plain.src_ref,
                dst_ref=relay.at[0, pl.ds(chunk_at(n) * ROWS, ROWS)],
                send_sem=lat_send.at[side, n],
                recv_sem=relay_recv.at[0, n],
                device_id=across,
                device_id_type=pl.DeviceIdType.MESH,
            ).start()

        @pl.when(jnp.logical_not(leaves))
        def _():
            plain.start()

    def relay_copy(t, stage, n, arrives, target=None):
        rows = pl.ds(chunk_at(n) * ROWS, ROWS)
        return pltpu.make_async_remote_copy(
            src_ref=relay.at[stage, rows],
            dst_ref=lat_halo.at[t % 2, mine, rows] if arrives else relay.at[1, rows],
            send_sem=relay_send.at[stage, n],
            recv_sem=lat_recv.at[t % 2, mine, n] if arrives else relay_recv.at[1, n],
            device_id=target or (onward if stage else turned),
            device_id_type=pl.DeviceIdType.MESH,
        )

    def relay_landed(stage, n):
        rows = pl.ds(chunk_at(n) * ROWS, ROWS)
        pltpu.make_async_remote_copy(
            src_ref=relay.at[stage, rows],
            dst_ref=relay.at[stage, rows],
            send_sem=relay_send.at[stage, n],
            recv_sem=relay_recv.at[stage, n],
            device_id=lifted,
            device_id_type=pl.DeviceIdType.MESH,
        ).wait_recv()

    def send_on(t, stage, n):
        relay_landed(stage, n)
        if stage == 1:
            relay_copy(t, stage, n, True).start()
            return

        @pl.when(corner)
        def _():
            relay_copy(t, stage, n, True).start()

        @pl.when(jnp.logical_not(corner) & (n % 2 == 0))
        def _():
            relay_copy(t, stage, n, False, turned).start()

        @pl.when(jnp.logical_not(corner) & (n % 2 == 1))
        def _():
            relay_copy(t, stage, n, False, lifted).start()

    def relays(s, n):
        for stage, lead in enumerate(LEADS):
            ahead = n + lead
            there = held(stage, ahead)
            here = there & (ahead < chunks)

            @pl.when(here)
            def _():
                send_on(s, stage, ahead)

            if s < STEPS - 1:
                @pl.when(there & (ahead >= chunks))
                def _():
                    send_on(s + 1, stage, ahead - chunks)

            left = n - SETTLE
            there = held(stage, left + chunks)

            @pl.when(there & (left >= 0))
            def _():
                relay_copy(s, stage, left, True).wait_send()

            if s > 0:

                @pl.when(there & (left < 0))
                def _():
                    relay_copy(s - 1, stage, left + chunks, True).wait_send()

    def lon_copy(t, side):
        row = width - 1 if side == LOW else 0
        src = field.at[:, row] if t == 0 else bufs[t % 2].at[:, row + 1]
        return pltpu.make_async_remote_copy(
            src_ref=src,
            dst_ref=bufs[t % 2].at[:, 0 if side == LOW else width + 1],
            send_sem=lon_send.at[t, side],
            recv_sem=lon_recv.at[t, side],
            device_id=lon_at[1 - side],
            device_id_type=pl.DeviceIdType.MESH,
        )

    def lev_copy(t, side, group):
        rows = pl.ds(group * (each * ROWS), each * ROWS)
        return pltpu.make_async_remote_copy(
            src_ref=lev_face.at[t, side, rows],
            dst_ref=lev_halo.at[t, side, rows],
            send_sem=lev_send.at[t, side, group],
            recv_sem=lev_recv.at[t, side, group],
            device_id=lev_at[1 - side],
            device_id_type=pl.DeviceIdType.MESH,
        )

    def lev_start(t, group):
        plain = lev_copy(t, HIGH, group)
        lev_copy(t, LOW, group).start()
        if t == 0:
            plain.start()
            return

        @pl.when(edge)
        def _():
            pltpu.make_async_remote_copy(
                src_ref=plain.src_ref,
                dst_ref=lev_pass.at[t, pl.ds(group * (each * ROWS), each * ROWS)],
                send_sem=lev_send.at[t, HIGH, group],
                recv_sem=pass_recv.at[t, group],
                device_id=aslant,
                device_id_type=pl.DeviceIdType.MESH,
            ).start()

        @pl.when(jnp.logical_not(edge))
        def _():
            plain.start()

    def pass_copy(t, group, landing=False):
        rows = pl.ds(group * (each * ROWS), each * ROWS)
        return pltpu.make_async_remote_copy(
            src_ref=lev_pass.at[t, rows],
            dst_ref=lev_pass.at[t, rows] if landing else lev_halo.at[t, HIGH, rows],
            send_sem=pass_send.at[t, group],
            recv_sem=pass_recv.at[t, group] if landing else lev_recv.at[t, HIGH, group],
            device_id=inward,
            device_id_type=pl.DeviceIdType.MESH,
        )

    def pass_on(s, n):
        for t, since in ((s + 1, n - each - PASS), (s, n + chunks - each - PASS)):
            if 0 < t < STEPS:
                here = (since >= 0) & (since % each == 0) & (since < chunks)

                @pl.when(here & jnp.logical_not(edge))
                def _():
                    pass_copy(t, since // each, True).wait_recv()
                    pass_copy(t, since // each).start()

    def both(copy, *where):
        return [copy(*(where[:1] + (side,) + where[1:])) for side in (LOW, HIGH)]

    load_field.start()
    load_crowd.start()
    barrier = pltpu.get_barrier_semaphore()

    def greet(partners):
        for partner in partners:
            pl.semaphore_signal(
                barrier, inc=1, device_id=partner, device_id_type=pl.DeviceIdType.MESH
            )

    greet((*lat_at, *lon_at, lev_at[0], aslant))

    @pl.when(edge)
    def _():
        greet((across, turned, lifted))

    pl.semaphore_wait(barrier, jnp.where(edge, 9, 6))

    for copy in both(lon_copy, 0):
        copy.start()

    def launch(n, carry):
        for side in (LOW, HIGH):
            lat_start(0, side, n)
        return carry

    lax.fori_loop(0, AHEAD, launch, 0)
    load_field.wait()

    def pack(position, carry):
        n = position // ROWS
        row = chunk_at(n) * ROWS + position % ROWS + 1
        for plane in range(depth):
            lev_face[0, LOW, position, pl.ds(plane, 1)] = even[plane, row, pl.ds(tall - 1, 1)]
            lev_face[0, HIGH, position, pl.ds(plane, 1)] = even[plane, row, pl.ds(0, 1)]
        return carry

    lax.fori_loop(0, width, pack, 0)
    for group in range(GROUPS):
        for copy in both(lev_copy, 0, group):
            copy.start()
    load_crowd.wait()

    for stage, lead in enumerate(LEADS):

        def begin(n, carry, stage=stage):
            @pl.when(held(stage, n))
            def _():
                send_on(0, stage, n)

            return carry

        lax.fori_loop(0, lead, begin, 0)

    place = lax.broadcasted_iota(jnp.int32, (8, 128), 0)

    def new_row(s, n, r):
        src, dst = bufs[s % 2], bufs[(s + 1) % 2]
        at = chunk_at(n) * ROWS + r
        row, position = at + 1, n * ROWS + r
        for plane in range(depth):
            for start, stop in ((0, 8), (8, 32), (32, 64), (64, tall - 8), (tall - 8, tall)):
                span = pl.ds(start, stop - start)
                middle = src[plane, row, span]
                if start == 0:
                    halo = lev_halo[s, LOW, position, pl.ds(plane, 1)]
                    lower = jnp.where(place == 0, halo, pltpu.roll(middle, 1, 0))
                else:
                    lower = src[plane, row, pl.ds(start - 1, stop - start)]
                if stop == tall:
                    halo = lev_halo[s, HIGH, position, pl.ds(plane, 1)]
                    upper = jnp.where(place == 7, halo, pltpu.roll(middle, 7, 0))
                else:
                    upper = src[plane, row, pl.ds(start + 1, stop - start)]
                around = lower + upper + src[plane, row - 1, span] + src[plane, row + 1, span]
                if plane == 0:
                    around += lat_halo[s % 2, LOW, at, span]
                else:
                    around += src[plane - 1, row, span]
                if plane == depth - 1:
                    around += lat_halo[s % 2, HIGH, at, span]
                else:
                    around += src[plane + 1, row, span]
                growth = 0.6 - 0.2 * (middle * crowd[plane, at, span])
                new = 0.1 * around + middle * growth
                if s == STEPS - 1:
                    crowd[plane, at, span] = new
                else:
                    dst[plane, row, span] = new
                if s < STEPS - 1:
                    if start == 0:
                        lev_face[s + 1, HIGH, position, pl.ds(plane, 1)] = new[0:1]
                    if stop == tall:
                        lev_face[s + 1, LOW, position, pl.ds(plane, 1)] = new[7:8]

    for s in range(STEPS):

        def chunk(n, carry, s=s):
            relays(s, n)
            pass_on(s, n)
            for copy in both(lat_copy, s, n):
                copy.wait_recv()

            @pl.when(n + AHEAD < chunks)
            def _():
                if s > 0:
                    for copy in both(lat_copy, s - 1, n + AHEAD):
                        copy.wait_send()
                for side in (LOW, HIGH):
                    lat_start(s, side, n + AHEAD)

            if s < STEPS - 1:

                @pl.when(n + AHEAD >= chunks)
                def _():
                    for copy in both(lat_copy, s, n + AHEAD - chunks):
                        copy.wait_send()
                    for side in (LOW, HIGH):
                        lat_start(s + 1, side, n + AHEAD - chunks)

            @pl.when(n == 0)
            def _():
                if s > 0:
                    lev_start(s, GROUPS - 1)
                    for copy in both(lon_copy, s - 1):
                        copy.wait_send()
                for copy in both(lon_copy, s):
                    copy.wait_recv()

            if s < STEPS - 1:

                @pl.when(n == 2)
                def _():
                    for copy in both(lon_copy, s + 1):
                        copy.start()

            @pl.when(n % each == 0)
            def _():
                for copy in both(lev_copy, s, n // each):
                    copy.wait_recv()
                if s < STEPS - 1:

                    @pl.when(n > 0)
                    def _():
                        lev_start(s + 1, n // each - 1)

            def row(r, inner):
                new_row(s, n, r)
                return inner

            return lax.fori_loop(0, ROWS, row, carry)

        lax.fori_loop(0, chunks, chunk, 0)

    def drain(n, carry):
        for copy in both(lat_copy, STEPS - 1, n):
            copy.wait_send()
        return carry

    for copy in both(lon_copy, STEPS - 1):
        copy.wait_send()
    for t in range(STEPS):
        for group in range(GROUPS):
            for copy in both(lev_copy, t, group):
                copy.wait_send()
    lax.fori_loop(0, chunks, drain, 0)

    @pl.when(jnp.logical_not(edge))
    def _():
        for t in range(1, STEPS):
            for group in range(GROUPS):
                pass_copy(t, group).wait_send()

    for stage in (0, 1):

        def settle(n, carry, stage=stage):
            @pl.when(held(stage, n))
            def _():
                relay_copy(STEPS - 1, stage, n, True).wait_send()

            return carry

        lax.fori_loop(chunks - SETTLE, chunks, settle, 0)


def local(field, crowding):
    depth, width, tall, lanes = field.shape
    chunks = width // ROWS
    padded = (depth, width + 2, tall, lanes)
    faces = (STEPS, 2, width, depth, lanes)
    dma = pltpu.SemaphoreType.DMA
    return pl.pallas_call(
        kernel,
        out_shape=pltpu.VMEM(field.shape, field.dtype),
        in_specs=[pl.BlockSpec(memory_space=pl.ANY)] * 2,
        out_specs=pl.BlockSpec(memory_space=pltpu.VMEM),
        scratch_shapes=[
            pltpu.VMEM(padded, jnp.float32),
            pltpu.VMEM(padded, jnp.float32),
            pltpu.VMEM((2, 2, width, tall, lanes), jnp.float32),
            pltpu.VMEM(faces, jnp.float32),
            pltpu.VMEM(faces, jnp.float32),
            pltpu.VMEM((2, width, tall, lanes), jnp.float32),
            pltpu.VMEM((STEPS, width, depth, lanes), jnp.float32),
            dma((2,)),
            dma((2, chunks)),
            dma((2, 2, chunks)),
            dma((STEPS, 2)),
            dma((STEPS, 2)),
            dma((STEPS, 2, GROUPS)),
            dma((STEPS, 2, GROUPS)),
            dma((2, chunks)),
            dma((2, chunks)),
            dma((STEPS, GROUPS)),
            dma((STEPS, GROUPS)),
        ],
        compiler_params=pltpu.CompilerParams(
            collective_id=0, has_side_effects=True, vmem_limit_bytes=46 * 1024 * 1024
        ),
        name="march",
    )(field, crowding)


def solution(mesh):
    spec = P("lat", "lon", "lev", None)
    return jax.shard_map(
        local, mesh=mesh, in_specs=(spec, spec), out_specs=spec, check_vma=False
    )
```
